32 devices in a mesh: dp: 8 (over z, y), tensor: 4 (over x, core).
Axes of the slice: x: 2, y: 2, z: 4, core: 2. Of those that a mesh axis runs over, the one named last changes fastest.
Arguments:
- acts: bfloat16 [8, 2048, 1024], P('dp', 'tensor'), may hold values from -6 to 6
- grad_out: bfloat16 [8, 2048, 1024], P('dp', 'tensor'), may hold values from -6 to 6
- norm_gain: float32 [1024], replicated, may hold values from 0.5 to 1.5
- w_zx: bfloat16 [1024, 2, 2048], P('dp', None, 'tensor'), may hold values from -0.1875 to 0.1875
- w_bc: bfloat16 [1024, 256], P('dp'), may hold values from -0.1875 to 0.1875
- w_dt: bfloat16 [1024, 32], P('dp', 'tensor'), may hold values from -0.1875 to 0.1875
- w_out: bfloat16 [1024, 2048], P('dp', 'tensor'), may hold values from -0.125 to 0.125
- conv_x: float32 [4, 2048], replicated, may hold values from -3 to 3
- conv_x_bias: float32 [2048], replicated, may hold values from -0.5 to 0.5
- conv_bc: float32 [4, 256], replicated, may hold values from -3 to 3
- conv_bc_bias: float32 [256], replicated, may hold values from -0.5 to 0.5
- dt_bias: float32 [32], replicated, may hold values from -7 to -2
- a_log: float32 [32], replicated, may hold values from 0 to 2.77
- d_skip: float32 [32], replicated, may hold values from 0.5 to 1.5
- gate_gain: float32 [2048], replicated, may hold values from 0.5 to 1.5
Outputs:
- out_acts: bfloat16 [8, 2048, 1024], P('dp', 'tensor')
- grad_acts: float32 [8, 2048, 1024], P('dp', 'tensor')
- grad_norm_gain: float32 [1024], replicated
- grad_w_zx: float32 [1024, 2, 2048], P('dp', None, 'tensor')
- grad_w_bc: float32 [1024, 256], P('dp')
- grad_w_dt: float32 [1024, 32], P('dp', 'tensor')
- grad_w_out: float32 [1024, 2048], P('dp', 'tensor')
- grad_conv_x: float32 [4, 2048], replicated
- grad_conv_x_bias: float32 [2048], replicated
- grad_conv_bc: float32 [4, 256], replicated
- grad_conv_bc_bias: float32 [256], replicated
- grad_dt_bias: float32 [32], replicated
- grad_a_log: float32 [32], replicated
- grad_d_skip: float32 [32], replicated
- grad_gate_gain: float32 [2048], replicated
The draws below stay inside these ranges and needn't reach their ends.
All inputs are finite; a program needn't handle non-finite values.
Results may differ from the reference program's by a relative error of at most 0.0096.
Values may be sent and summed in bfloat16 or wider, within the bound.
A program may use at most 192 MiB of HBM per device.

```python
import jax
import jax.numpy as jnp
from jax import lax

D = 1024
DI = 2048
H = 32
N = 128
K = 4
BLOCK_LEN = 256
SEQ = 2048
BATCH = 8


def spiked(values, key, source, target, shards_of, factor):
    def block_of(axis_at):
        return (jnp.arange(values.shape[axis_at]) // (values.shape[axis_at] // shards_of)).reshape((-1,) + (1,) * (values.ndim - 1 - axis_at))

    near = jax.random.permutation(key, shards_of)[block_of(target)]
    other_side = (block_of(target) + shards_of // 2) % shards_of
    return jnp.where((block_of(source) == near) | (block_of(source) == other_side), factor * values, values)


def block_levels(key, extent, pieces, smallest, top_value):
    def one(dim, parts):
        heights = jax.random.uniform(jax.random.fold_in(jax.random.fold_in(key, 6), dim), (parts,), jnp.float32, smallest / len(pieces), top_value / len(pieces))
        return jnp.repeat(jnp.exp(heights), extent[dim] // parts).reshape((-1,) + (1,) * (len(extent) - dim - 1))

    gain = one(*pieces[0])
    for cut in pieces[1:]:
        gain = gain * one(*cut)
    return gain


def bell_draw(stream_key, extent, scale, most, pieces=(), held_as=jnp.bfloat16):
    values = jax.random.normal(stream_key, extent, jnp.float32) * scale
    if len(pieces) > 0:
        values = block_levels(stream_key, extent, pieces, -0.22, 0.18) * values
    return jnp.clip(values, min=-most, max=most).astype(held_as)


def noise_with(key, shape, scale, bound, shards, heavy, held_as=jnp.bfloat16):
    values = scale * jax.random.normal(key, shape, jnp.float32)
    if shards:
        values = values * block_levels(key, shape, shards, -0.22, 0.18)
    return jnp.clip(spiked(values, jax.random.fold_in(key, 3), *heavy), -bound, bound).astype(held_as)


def setup_inputs(seed: int = 0) -> dict:
    seeds = jax.random.split(jax.random.key(seed), 16)
    return {
        "acts": noise_with(seeds[0], (BATCH, SEQ, D), 1.0, 6.0, ((0, 8), (1, 4)), (0, 2, 8, 2.0)),
        "grad_out": noise_with(seeds[1], (BATCH, SEQ, D), 1.0, 6.0, ((0, 8), (1, 4)), (0, 2, 8, 2.0)),
        "norm_gain": jnp.clip(1.0 + 0.1 * jax.random.normal(seeds[2], (D,), jnp.float32), 0.5, 1.5),
        "w_zx": bell_draw(seeds[3], (D, 2, DI), D ** -0.5, 0.1875, ((0, 8), (2, 4))),
        "w_bc": bell_draw(seeds[4], (D, 2 * N), D ** -0.5, 0.1875, ((0, 8),)),
        "w_dt": bell_draw(seeds[5], (D, H), D ** -0.5, 0.1875, ((0, 8), (1, 4))),
        "w_out": bell_draw(seeds[6], (D, DI), DI ** -0.5, 0.125, ((0, 8), (1, 4))),
        "conv_x": bell_draw(seeds[7], (K, DI), 0.5, 3.0, (), jnp.float32),
        "conv_x_bias": jnp.clip(jax.random.uniform(seeds[8], (DI,), jnp.float32, -0.5, 0.5), -0.5, 0.5),
        "conv_bc": bell_draw(seeds[9], (K, 2 * N), 0.5, 3.0, (), jnp.float32),
        "conv_bc_bias": jnp.clip(jax.random.uniform(seeds[10], (2 * N,), jnp.float32, -0.5, 0.5), -0.5, 0.5),
        "dt_bias": jnp.clip(jax.random.uniform(seeds[11], (H,), jnp.float32, -7.0, -2.0), -7.0, -2.0),
        "a_log": jnp.clip(jax.random.uniform(seeds[12], (H,), jnp.float32, 0.0, 2.77), 0.0, 2.77),
        "d_skip": jnp.clip(jax.random.uniform(seeds[13], (H,), jnp.float32, 0.5, 1.5), 0.5, 1.5),
        "gate_gain": jnp.clip(1.0 + 0.1 * jax.random.normal(seeds[14], (DI,), jnp.float32), 0.5, 1.5),
    }


EPSILON = 1e-05
FULL_PRECISION = lax.Precision.HIGHEST

@jax.custom_vjp
def low(v):
    return lax.optimization_barrier(v.astype(jnp.bfloat16)).astype(jnp.float32)

@jax.custom_vjp
def low_back(v):
    return v

def low_keep(v):
    return (low(v), None)

def low_pass(kept, grad):
    return (grad,)

def back_keep(v):
    return (v, None)

def back_low(kept, grad):
    return (low(grad),)
low.defvjp(low_keep, low_pass)
low_back.defvjp(back_keep, back_low)

def causal_conv(values, conv_taps):
    tap_count = conv_taps.shape[0]
    length = values.shape[0]
    padded = jnp.pad(values, ((tap_count - 1, 0), (0, 0)))
    result = conv_taps[0] * padded[0:length]
    for offset in range(1, tap_count):
        result = result + conv_taps[offset] * padded[offset:offset + length]
    return result

def ssd_scan(x_heads, step_dt, decay_rate, b_mat, c_mat, block_size):
    length, head_count, head_width = x_heads.shape
    state_count = b_mat.shape[1]
    block_count = length // block_size
    x_blocks = x_heads.reshape(block_count, block_size, head_count, head_width)
    dt_blocks = step_dt.reshape(block_count, block_size, head_count)
    b_blocks = b_mat.reshape(block_count, block_size, state_count)
    c_blocks = c_mat.reshape(block_count, block_size, state_count)
    positions = jnp.arange(block_size)
    causal_mask = (positions[:, None] >= positions[None, :]).astype(jnp.float32)

    def step_block(state, inputs):
        x_block, dt_block, b_block, c_block = inputs
        cum_logs = jnp.cumsum(dt_block * decay_rate[None, :], axis=0)
        scores = jnp.dot(c_block, b_block.T, precision=FULL_PRECISION)
        log_gaps = (cum_logs[:, None, :] - cum_logs[None, :, :]) * causal_mask[:, :, None]
        weights = scores[:, :, None] * jnp.exp(log_gaps) * causal_mask[:, :, None] * dt_block[None, :, :]
        within = jnp.einsum('ijh,jhp->ihp', weights, x_block, precision=FULL_PRECISION)
        carried = jnp.einsum('in,hpn->ihp', c_block, state, precision=FULL_PRECISION) * jnp.exp(cum_logs)[:, :, None]
        block_total = cum_logs[-1]
        state_weight = jnp.exp(block_total[None, :] - cum_logs) * dt_block
        update = jnp.einsum('jhp,jn->hpn', x_block * state_weight[:, :, None], b_block, precision=FULL_PRECISION)
        new_state = state * jnp.exp(block_total)[:, None, None] + update
        return (new_state, within + carried)
    zero_state = jnp.zeros((head_count, head_width, state_count), jnp.float32)
    final_state, outputs = lax.scan(jax.checkpoint(step_block), zero_state, (x_blocks, dt_blocks, b_blocks, c_blocks))
    return outputs.reshape(length, head_count, head_width)

def layer(acts_row, params):
    norm_gain, w_zx, w_bc, w_dt, w_out, conv_x, conv_x_bias, conv_bc, conv_bc_bias, dt_bias, a_log, d_skip, gate_gain = params
    length = acts_row.shape[0]
    head_count = w_dt.shape[1]
    state_count = w_bc.shape[1] // 2
    normed_in = acts_row * lax.rsqrt(lax.optimization_barrier(jnp.mean(acts_row * acts_row, axis=-1, keepdims=True)) + EPSILON) * norm_gain
    hidden = low(normed_in)
    gate_in = low_back(jnp.dot(hidden, w_zx[:, 0, :], precision=FULL_PRECISION))
    x_in = low_back(jnp.dot(hidden, w_zx[:, 1, :], precision=FULL_PRECISION))
    bc_in = low_back(jnp.dot(hidden, w_bc, precision=FULL_PRECISION))
    dt_in = low_back(jnp.dot(hidden, w_dt, precision=FULL_PRECISION))
    x_conv = jax.nn.silu(causal_conv(x_in, conv_x) + conv_x_bias)
    bc_conv = jax.nn.silu(causal_conv(bc_in, conv_bc) + conv_bc_bias)
    x_heads = low(x_conv).reshape(length, head_count, -1)
    b_mat = low(bc_conv[:, :state_count])
    c_mat = low(bc_conv[:, state_count:])
    step_dt = jax.nn.softplus(dt_in + dt_bias)
    decay_rate = -jnp.exp(a_log)
    mixed = ssd_scan(x_heads, step_dt, decay_rate, b_mat, c_mat, BLOCK_LEN) + d_skip[None, :, None] * x_heads
    gated = mixed.reshape(length, -1) * jax.nn.silu(gate_in)
    normed = gated * lax.rsqrt(lax.optimization_barrier(jnp.mean(gated * gated, axis=-1, keepdims=True)) + EPSILON) * gate_gain
    mixed_out = low_back(low(normed))
    return acts_row + jnp.dot(mixed_out, w_out.T, precision=FULL_PRECISION)

def add_pair(first_item, second_item):
    return first_item + second_item

def reference(acts, grad_out, norm_gain, w_zx, w_bc, w_dt, w_out, conv_x, conv_x_bias, conv_bc, conv_bc_bias, dt_bias, a_log, d_skip, gate_gain):
    params = tuple((item.astype(jnp.float32) for item in (norm_gain, w_zx, w_bc, w_dt, w_out, conv_x, conv_x_bias, conv_bc, conv_bc_bias, dt_bias, a_log, d_skip, gate_gain)))

    def one_sequence(totals, inputs):
        acts_row, grad_row = inputs
        result, backward = jax.vjp(layer, acts_row.astype(jnp.float32), params)
        grad_input, grad_params = backward(grad_row.astype(jnp.float32))
        totals = jax.tree.map(add_pair, totals, grad_params)
        return (totals, (result.astype(jnp.bfloat16), grad_input))
    zero_totals = jax.tree.map(jnp.zeros_like, params)
    totals, outputs = lax.scan(one_sequence, zero_totals, (acts, grad_out))
    out_acts, grad_acts = outputs
    return (out_acts, grad_acts, totals[0], totals[1], totals[2], totals[3], totals[4], totals[5], totals[6], totals[7], totals[8], totals[9], totals[10], totals[11], totals[12])
```

```python
import functools

import jax
import jax.numpy as jnp
from jax import lax
from jax.experimental import pallas as pl
from jax.experimental.pallas import tpu as pltpu
from jax.sharding import PartitionSpec as P

BLOCK_LEN = 256
EPSILON = 1e-05
LANES = 128
HALO = 8
FAR = -1e30
F32 = jnp.float32
BF16 = jnp.bfloat16
CONTRACT_LAST = (((1,), (1,)), ((), ()))
CONTRACT_FIRST = (((0,), (0,)), ((), ()))


def mm(a, b):
    return jnp.dot(a, b, preferred_element_type=F32)


def mm_nt(a, b):
    return lax.dot_general(a, b, CONTRACT_LAST, preferred_element_type=F32)


def mm_tn(a, b):
    return lax.dot_general(a, b, CONTRACT_FIRST, preferred_element_type=F32)


def split_two(v):
    high = v.astype(BF16)
    return high, (v - high.astype(F32)).astype(BF16)


def split_three(v):
    first = v.astype(BF16)
    rest = v - first.astype(F32)
    second = rest.astype(BF16)
    return first, second, (rest - second.astype(F32)).astype(BF16)


def lanes_of(shape):
    return lax.broadcasted_iota(jnp.int32, shape, 1)


def rows_of(shape):
    return lax.broadcasted_iota(jnp.int32, shape, 0)


def spread_heads(v, spread, heads):
    first, second, third = split_three(v)
    lane = lanes_of(v.shape)
    packed = jnp.where(lane < heads, first.astype(F32), second.astype(F32))
    packed = jnp.where(lane < 2 * heads, packed, third.astype(F32))
    return mm(packed.astype(BF16), spread)


def head_sums(v, gather):
    high, low = split_two(v)
    return mm(high, gather) + mm(low, gather)


def tri_sums(tri, v):
    first, second, third = split_three(v)
    return mm(tri, first) + mm(tri, second) + mm(tri, third)


def spread_matrix(heads, channels):
    lane = rows_of((LANES, channels))
    head = lanes_of((LANES, channels)) // (channels // heads)
    return jnp.where((lane < 3 * heads) & (lane % heads == head), 1.0, 0.0).astype(BF16)


def gather_matrix(heads, channels):
    head = rows_of((channels, LANES)) // (channels // heads)
    return jnp.where(lanes_of((channels, LANES)) % heads == head, 1.0, 0.0).astype(BF16)


def conv_pre(buf, taps, length, tap_count):
    pre = taps[tap_count : tap_count + 1]
    for k in range(tap_count):
        pre = pre + taps[k : k + 1] * buf[pl.ds(HALO - tap_count + 1 + k, length), :]
    return pre


def fill(buf, prev_ref, cur_ref, is_first):
    prev = prev_ref[...]
    buf[0:HALO, :] = jnp.where(is_first, jnp.zeros_like(prev), prev)
    buf[HALO:, :] = cur_ref[...]


def step_values(dt_ref, ph):
    shifted = dt_ref[...] + ph[0:1]
    step_dt = jnp.maximum(shifted, 0.0) + jnp.log1p(jnp.exp(-jnp.abs(shifted)))
    log_step = step_dt * ph[1:2]
    return shifted, step_dt, log_step


def fwd_kernel(heads, gate_ref, xprev_ref, x_ref, bcprev_ref, bc_ref, dt_ref, gm_ref, px_ref, pbc_ref, ph_ref,
               mixed_ref, states_ref, sums_ref, xbuf, bcbuf, state, y_ref):
    step = pl.program_id(0)
    is_first = step == 0
    length, channels = x_ref.shape
    half = length // 2
    state_count = bc_ref.shape[1] // 2
    width = channels // heads

    @pl.when(is_first)
    def _():
        state[...] = jnp.zeros_like(state)

    fill(xbuf, xprev_ref, x_ref, is_first)
    fill(bcbuf, bcprev_ref, bc_ref, is_first)
    px, pbc, ph = px_ref[...], pbc_ref[...], ph_ref[...]
    x_low = jax.nn.silu(conv_pre(xbuf, px, length, 4)).astype(BF16)
    bc_low = jax.nn.silu(conv_pre(bcbuf, pbc, length, 4)).astype(BF16)
    b_low, c_low = bc_low[:, :state_count], bc_low[:, state_count:]
    _, step_dt, log_step = step_values(dt_ref, ph)
    tri = (rows_of((length, length)) >= lanes_of((length, length))).astype(F32).astype(BF16)
    cum = tri_sums(tri, log_step)
    cum_t = cum.T
    dt_t = step_dt.T
    spread = spread_matrix(heads, channels)
    exp_cum = spread_heads(jnp.exp(cum), spread, heads)
    weight = spread_heads(jnp.exp(cum[length - 1 : length] - cum) * step_dt, spread, heads)

    scores = mm_nt(c_low, b_low)
    lane = lanes_of((length, LANES))
    per_lane = LANES // width
    for group in range(heads // per_lane):
        cols = slice(group * LANES, (group + 1) * LANES)
        xp = x_low[:, cols]
        top = jnp.zeros((half, LANES), F32)
        bottom = jnp.zeros((half, LANES), F32)
        for s in range(per_lane):
            h = group * per_lane + s
            xm = jnp.where(lane // width == s, xp, jnp.zeros_like(xp))
            for part in range(2):
                r0, cn = part * half, (part + 1) * half
                rows = slice(r0, r0 + half)
                gaps = cum[rows, h : h + 1] - cum_t[h : h + 1, :cn]
                shape = (half, cn)
                keep = rows_of(shape) + r0 >= lanes_of(shape)
                decay = jnp.exp(jnp.where(keep, gaps, FAR))
                w = (scores[rows, :cn] * decay * dt_t[h : h + 1, :cn]).astype(BF16)
                if part == 0:
                    top = top + mm(w, xm[:cn])
                else:
                    bottom = bottom + mm(w, xm[:cn])
        y_ref[0:half, cols] = top
        y_ref[half:, cols] = bottom

    old = state[...]
    states_ref[0] = old
    old_high, old_low = split_two(old)
    carried = mm(c_low, old_high) + mm(c_low, old_low)
    x_wide = x_low.astype(F32)
    xw_high, xw_low = split_two(x_wide * weight)
    state[...] = old * exp_cum[length - 1 : length] + (mm_tn(b_low, xw_high) + mm_tn(b_low, xw_low))
    mixed = y_ref[...] + carried * exp_cum + px[6:7] * x_wide
    mixed_ref[...] = mixed
    gated = mixed * jax.nn.silu(gate_ref[...])
    squares = jnp.sum(gated * gated, axis=1, keepdims=True)
    inner = jnp.sum(gm_ref[...].astype(F32) * px[5:6] * gated, axis=1, keepdims=True)
    both = jnp.where(lane == 0, squares, jnp.where(lane == 1, inner, 0.0))
    sums_ref[0] = both.T[:8]


def bwd_kernel(heads, gate_ref, xprev_ref, x_ref, bcprev_ref, bc_ref, dt_ref, gm_ref, mixed_ref, states_ref, stats_ref,
               px_ref, pbc_ref, ph_ref, g_ref, gx_ref, gbc_ref, gh_ref, xbuf, bcbuf, gxbuf, gbcbuf, dstate, dx_ref, dg_ref):
    step = pl.program_id(0)
    is_first = step == pl.num_programs(0) - 1
    length, channels = x_ref.shape
    half = length // 2
    state_count = bc_ref.shape[1] // 2
    width = channels // heads

    @pl.when(step == 0)
    def _():
        dstate[...] = jnp.zeros_like(dstate)
        gxbuf[...] = jnp.zeros_like(gxbuf)
        gbcbuf[...] = jnp.zeros_like(gbcbuf)
        gx_ref[...] = jnp.zeros_like(gx_ref)
        gbc_ref[...] = jnp.zeros_like(gbc_ref)
        gh_ref[...] = jnp.zeros_like(gh_ref)

    fill(xbuf, xprev_ref, x_ref, is_first)
    fill(bcbuf, bcprev_ref, bc_ref, is_first)
    px, pbc, ph = px_ref[...], pbc_ref[...], ph_ref[...]
    pre_x = conv_pre(xbuf, px, length, 4)
    sig_x = jax.nn.sigmoid(pre_x)
    x_low = (pre_x * sig_x).astype(BF16)
    slope_x = sig_x * (1.0 + pre_x * (1.0 - sig_x))
    pre_bc = conv_pre(bcbuf, pbc, length, 4)
    sig_bc = jax.nn.sigmoid(pre_bc)
    bc_low = (pre_bc * sig_bc).astype(BF16)
    slope_bc = sig_bc * (1.0 + pre_bc * (1.0 - sig_bc))
    b_low, c_low = bc_low[:, :state_count], bc_low[:, state_count:]
    shifted, step_dt, log_step = step_values(dt_ref, ph)
    tri = (rows_of((length, length)) >= lanes_of((length, length))).astype(F32).astype(BF16)
    cum = tri_sums(tri, log_step)
    cum_t = cum.T
    spread = spread_matrix(heads, channels)
    gather = gather_matrix(heads, channels)
    exp_cum = spread_heads(jnp.exp(cum), spread, heads)
    weight = spread_heads(jnp.exp(cum[length - 1 : length] - cum) * step_dt, spread, heads)
    dt_wide = spread_heads(step_dt, spread, heads)
    x_wide = x_low.astype(F32)

    stats = stats_ref[0]
    stats = jnp.concatenate([stats, jnp.zeros((LANES - 8, length), F32)], axis=0).T
    rs, coef = stats[:, 0:1], stats[:, 1:2]
    gate = gate_ref[...]
    sig = jax.nn.sigmoid(gate)
    silu = gate * sig
    mixed = mixed_ref[...]
    gated = mixed * silu
    gm = gm_ref[...].astype(F32)
    ggated = rs * (gm * px[5:6]) - gated * coef
    d_gain = jnp.sum(gm * gated * rs, axis=0, keepdims=True)
    dy = ggated * silu
    g_ref[:, 0:channels] = (ggated * mixed * (sig * (1.0 + gate * (1.0 - sig)))).astype(BF16)
    dy_low = dy.astype(BF16)
    d_skip = jnp.sum(dy * x_wide, axis=0, keepdims=True)

    old = states_ref[0]
    old_high, old_low = split_two(old)
    ds = dstate[...]
    ds_high, ds_low = split_two(ds)
    dye = dy * exp_cum
    dye_low = dye.astype(BF16)
    dc = mm_nt(dye_low, old_high)
    carried = mm(c_low, old_high) + mm(c_low, old_low)
    from_carried = head_sums(dye * carried, gather)
    dxs = (mm(b_low, ds_high) + mm(b_low, ds_low)) * weight
    from_state = head_sums(x_wide * dxs, gather)
    db = mm_nt((x_wide * weight).astype(BF16), ds_high)
    last = exp_cum[length - 1 : length]
    decayed = jnp.sum(old * ds, axis=0, keepdims=True) * last
    decayed = head_sums(jnp.broadcast_to(decayed, (8, channels)), gather)[0:1]
    dstate[...] = ds * last + mm_tn(c_low, dye_low)

    scores = mm_nt(b_low, c_low)
    xdt_low = (x_wide * dt_wide).astype(BF16)
    lane = lanes_of((length, LANES))
    per_lane = LANES // width
    dg_ref[...] = jnp.zeros_like(dg_ref)
    col_sums = jnp.zeros((length, LANES), F32)
    row_sums = jnp.zeros((8, length), F32)
    row8 = rows_of((8, length))
    for group in range(heads // per_lane):
        cols = slice(group * LANES, (group + 1) * LANES)
        xp, dyp = xdt_low[:, cols], dy_low[:, cols]
        top = jnp.zeros((half, LANES), F32)
        bottom = jnp.zeros((half, LANES), F32)
        for s in range(per_lane):
            h = group * per_lane + s
            mine = lane // width == s
            xm = jnp.where(mine, xp, jnp.zeros_like(xp))
            dym = jnp.where(mine, dyp, jnp.zeros_like(dyp))
            col_parts = []
            row_parts = []
            for part in range(2):
                r0 = part * half
                rows = slice(r0, r0 + half)
                gaps = cum_t[h : h + 1, r0:] - cum[rows, h : h + 1]
                shape = (half, length - r0)
                keep = lanes_of(shape) >= rows_of(shape)
                decay = jnp.exp(jnp.where(keep, gaps, FAR))
                v = scores[rows, r0:] * decay
                dw = mm_nt(xm[rows], dyp[r0:])
                dg_ref[rows, r0:] += decay * dw
                e = v * dw
                col_parts.append(jnp.sum(e, axis=1, keepdims=True))
                row_parts.append(jnp.sum(e, axis=0, keepdims=True))
                if part == 0:
                    top = top + mm(v.astype(BF16), dym)
                else:
                    bottom = bottom + mm(v.astype(BF16), dym[r0:])
            col = jnp.concatenate(col_parts, axis=0)
            row = row_parts[0] + jnp.concatenate([jnp.zeros((1, half), F32), row_parts[1]], axis=1)
            col_sums = jnp.where(lane % heads == h, col, col_sums)
            row_sums = jnp.where(row8 == h, row, row_sums)
        dx_ref[0:half, cols] = top
        dx_ref[half:, cols] = bottom

    dg_low = dg_ref[...].astype(BF16)
    db = db + mm(dg_low, c_low)
    dc = dc + mm_tn(dg_low, b_low)
    dx = dx_ref[...] * dt_wide + dxs + px[6:7] * dy

    row_cols = jnp.concatenate([row_sums] * (LANES // 8), axis=0).T
    local = row_cols - col_sums + from_carried - from_state
    tri_up = (rows_of((length, length)) <= lanes_of((length, length))).astype(F32).astype(BF16)
    grad_log = tri_sums(tri_up, local) + (jnp.sum(from_state, axis=0, keepdims=True) + decayed)
    direct = jnp.where(step_dt > 0.0, (col_sums + from_state) / step_dt, 0.0)
    grad_dt = (direct + ph[1:2] * grad_log) * jax.nn.sigmoid(shifted)
    gh_ref[0:1] += jnp.sum(grad_dt, axis=0, keepdims=True)
    gh_ref[1:2] += jnp.sum(grad_log * log_step, axis=0, keepdims=True)
    g_ref[:, 2 * channels + 2 * state_count :] = jnp.where(lane < heads, grad_dt, 0.0).astype(BF16)

    def conv_back(grad, slope, buf, gbuf, taps, sums_ref):
        gbuf[length:, :] = gbuf[0:HALO, :]
        gp = grad * slope
        gbuf[0:length, :] = gp
        result = jnp.zeros_like(gp)
        for k in range(4):
            result = result + taps[k : k + 1] * gbuf[pl.ds(3 - k, length), :]
            sums_ref[k : k + 1] += jnp.sum(buf[pl.ds(HALO - 3 + k, length), :] * gp, axis=0, keepdims=True)
        sums_ref[4:5] += jnp.sum(gp, axis=0, keepdims=True)
        return result.astype(BF16)

    g_ref[:, channels : 2 * channels] = conv_back(dx, slope_x, xbuf, gxbuf, px, gx_ref)
    g_ref[:, 2 * channels : 2 * channels + 2 * state_count] = conv_back(
        jnp.concatenate([db, dc], axis=1), slope_bc, bcbuf, gbcbuf, pbc, gbc_ref
    )
    gx_ref[5:6] += d_gain
    gx_ref[6:7] += d_skip


def scan_specs(length, channels, states, block):
    halo = length // HALO

    def at(width, start):
        return pl.BlockSpec((length, width), lambda i: (block(i), start // width))

    def before(width, start):
        return pl.BlockSpec((HALO, width), lambda i: (jnp.maximum(block(i) * halo - 1, 0), start // width))

    return [
        at(channels, 0),
        before(channels, channels),
        at(channels, channels),
        before(2 * states, 2 * channels),
        at(2 * states, 2 * channels),
        at(LANES, 2 * channels + 2 * states),
    ]


def whole(shape):
    return pl.BlockSpec(shape, lambda i: (0,) * len(shape))


def mix_forward(proj, grad_mixed, px, pbc, ph, heads):
    tokens, channels = grad_mixed.shape
    states = pbc.shape[1] // 2
    length = BLOCK_LEN
    blocks = tokens // length
    block = lambda i: i
    return pl.pallas_call(
        functools.partial(fwd_kernel, heads),
        grid=(blocks,),
        in_specs=scan_specs(length, channels, states, block)
        + [pl.BlockSpec((length, channels), lambda i: (i, 0)), whole(px.shape), whole(pbc.shape), whole(ph.shape)],
        out_specs=[
            pl.BlockSpec((length, channels), lambda i: (i, 0)),
            pl.BlockSpec((1, states, channels), lambda i: (i, 0, 0)),
            pl.BlockSpec((1, 8, length), lambda i: (i, 0, 0)),
        ],
        out_shape=[
            jax.ShapeDtypeStruct((tokens, channels), F32),
            jax.ShapeDtypeStruct((blocks, states, channels), F32),
            jax.ShapeDtypeStruct((blocks, 8, length), F32),
        ],
        scratch_shapes=[
            pltpu.VMEM((length + HALO, channels), F32),
            pltpu.VMEM((length + HALO, 2 * states), F32),
            pltpu.VMEM((states, channels), F32),
            pltpu.VMEM((length, channels), F32),
        ],
        name="mix_forward",
    )(proj, proj, proj, proj, proj, proj, grad_mixed, px, pbc, ph)


def mix_backward(proj, grad_mixed, mixed, states_in, stats, px, pbc, ph, heads):
    tokens, channels = grad_mixed.shape
    states = pbc.shape[1] // 2
    length = BLOCK_LEN
    blocks = tokens // length
    block = lambda i: blocks - 1 - i
    total = 2 * channels + 2 * states + LANES
    return pl.pallas_call(
        functools.partial(bwd_kernel, heads),
        grid=(blocks,),
        in_specs=scan_specs(length, channels, states, block)
        + [
            pl.BlockSpec((length, channels), lambda i: (block(i), 0)),
            pl.BlockSpec((length, channels), lambda i: (block(i), 0)),
            pl.BlockSpec((1, states, channels), lambda i: (block(i), 0, 0)),
            pl.BlockSpec((1, 8, length), lambda i: (block(i), 0, 0)),
            whole(px.shape),
            whole(pbc.shape),
            whole(ph.shape),
        ],
        out_specs=[
            pl.BlockSpec((length, total), lambda i: (block(i), 0)),
            whole((8, channels)),
            whole((8, 2 * states)),
            whole((8, LANES)),
        ],
        out_shape=[
            jax.ShapeDtypeStruct((tokens, total), BF16),
            jax.ShapeDtypeStruct((8, channels), F32),
            jax.ShapeDtypeStruct((8, 2 * states), F32),
            jax.ShapeDtypeStruct((8, LANES), F32),
        ],
        scratch_shapes=[
            pltpu.VMEM((length + HALO, channels), F32),
            pltpu.VMEM((length + HALO, 2 * states), F32),
            pltpu.VMEM((length + HALO, channels), F32),
            pltpu.VMEM((length + HALO, 2 * states), F32),
            pltpu.VMEM((states, channels), F32),
            pltpu.VMEM((length, channels), F32),
            pltpu.VMEM((length, length), F32),
        ],
        name="mix_backward",
    )(proj, proj, proj, proj, proj, proj, grad_mixed, mixed, states_in, stats, px, pbc, ph)


def widen(piece, start, full_size):
    holder = jnp.zeros(piece.shape[:-1] + (full_size,), F32)
    return lax.dynamic_update_slice_in_dim(holder, piece, start, piece.ndim - 1)


def body(acts, grad_out, norm_gain, w_zx, w_bc, w_dt, w_out, conv_x, conv_x_bias, conv_bc, conv_bc_bias,
         dt_bias, a_log, d_skip, gate_gain):
    parts = lax.axis_size("tensor")
    rank = lax.axis_index("tensor")
    rows, features = acts.shape[1:]
    w_rows, _, channels = w_zx.shape
    heads = w_dt.shape[1]
    states = w_bc.shape[1] // 2
    width = channels // heads
    total_channels, total_heads = channels * parts, heads * parts
    chan_start, head_start = rank * channels, rank * heads
    repeat = LANES // heads
    side = 2 * channels + 2 * states + LANES

    local_w = jnp.concatenate([w_zx.reshape(w_rows, 2 * channels), w_bc, jnp.tile(w_dt, (1, repeat)), w_out], axis=1)
    w_all = lax.all_gather(local_w, "dp", axis=0, tiled=True)
    w_in, w_o = w_all[:, :side], w_all[:, side:]

    acts_row = acts[0].astype(F32)
    rs0 = lax.rsqrt(jnp.mean(acts_row * acts_row, axis=-1, keepdims=True) + EPSILON)
    hidden = lax.all_gather((acts_row * rs0 * norm_gain).astype(BF16), "tensor", axis=0, tiled=True)
    grad_rows = lax.all_gather(grad_out[0], "tensor", axis=0, tiled=True)
    proj = mm(hidden, w_in)
    grad_mixed = mm(grad_rows, w_o).astype(BF16)

    def take(v, start, size):
        return lax.dynamic_slice_in_dim(v, start, size, v.ndim - 1)

    gain = take(gate_gain, chan_start, channels)
    skip = jnp.repeat(take(d_skip, head_start, heads), width)
    px = jnp.concatenate(
        [take(conv_x, chan_start, channels), take(conv_x_bias, chan_start, channels)[None], gain[None], skip[None],
         jnp.zeros((1, channels), F32)], axis=0)
    pbc = jnp.concatenate([conv_bc, conv_bc_bias[None], jnp.zeros((3, 2 * states), F32)], axis=0)
    ph = jnp.stack([jnp.tile(take(dt_bias, head_start, heads), repeat),
                    jnp.tile(-jnp.exp(take(a_log, head_start, heads)), repeat)])
    ph = jnp.concatenate([ph, jnp.zeros((6, LANES), F32)], axis=0)

    mixed, state_in, sums = mix_forward(proj, grad_mixed, px, pbc, ph, heads)
    sums = lax.psum(sums[:, :2], "tensor")
    inv = lax.rsqrt(sums[:, 0] / total_channels + EPSILON)
    coef = inv * inv * inv * (sums[:, 1] / total_channels)
    stats = jnp.concatenate([jnp.stack([inv, coef], axis=1), jnp.zeros((inv.shape[0], 6, inv.shape[1]), F32)], axis=1)
    mixed_out = (mixed * jax.nn.silu(proj[:, :channels]) * inv.reshape(-1, 1) * gain).astype(BF16)
    projected = lax.psum_scatter(mm_nt(mixed_out, w_o).astype(BF16), "tensor", scatter_dimension=0, tiled=True)
    out_acts = (acts_row + projected.astype(F32)).astype(BF16)[None]
    grad_w_out = lax.psum_scatter(mm_tn(grad_rows, mixed_out).astype(BF16), "dp", scatter_dimension=0, tiled=True)

    g_all, gx, gbc, gh = mix_backward(proj, grad_mixed, mixed, state_in, stats, px, pbc, ph, heads)
    grad_hidden = lax.psum_scatter(mm_nt(g_all, w_in).astype(BF16), "tensor", scatter_dimension=0, tiled=True)
    grad_w = lax.psum_scatter(mm_tn(hidden, g_all).astype(BF16), "dp", scatter_dimension=0, tiled=True).astype(F32)
    grad_w_bc = lax.psum(grad_w[:, 2 * channels : 2 * channels + 2 * states], "tensor")

    grad_hidden = grad_hidden.astype(F32)
    grad_ng = jnp.sum(grad_hidden * acts_row * rs0, axis=0)
    pulled = grad_hidden * norm_gain
    inner = jnp.sum(pulled * acts_row, axis=-1, keepdims=True)
    grad_acts = grad_out[0].astype(F32) + pulled * rs0 - acts_row * (rs0 * rs0 * rs0 / features * inner)

    pieces = (
        grad_ng,
        widen(gx[0:4], chan_start, total_channels),
        widen(gx[4], chan_start, total_channels),
        gbc[0:4],
        gbc[4],
        widen(gh[0, :heads], head_start, total_heads),
        widen(gh[1, :heads], head_start, total_heads),
        widen(jnp.sum(gx[6].reshape(heads, width), axis=1), head_start, total_heads),
        widen(gx[5], chan_start, total_channels),
    )
    ng, cx, cxb, cbc, cbcb, dtb, alog, dsk, gg = lax.psum(pieces, ("dp", "tensor"))
    return (
        out_acts,
        grad_acts[None],
        ng,
        grad_w[:, : 2 * channels].reshape(w_rows, 2, channels),
        grad_w_bc,
        grad_w[:, 2 * channels + 2 * states : 2 * channels + 2 * states + heads],
        grad_w_out.astype(F32),
        cx,
        cxb,
        cbc,
        cbcb,
        dtb,
        alog,
        dsk,
        gg,
    )


def solution(mesh):
    in_specs = (
        P("dp", "tensor", None),
        P("dp", "tensor", None),
        P(),
        P("dp", None, "tensor"),
        P("dp", None),
        P("dp", "tensor"),
        P("dp", "tensor"),
    ) + (P(),) * 8
    out_specs = (
        P("dp", "tensor", None),
        P("dp", "tensor", None),
        P(),
        P("dp", None, "tensor"),
        P("dp", None),
        P("dp", "tensor"),
        P("dp", "tensor"),
    ) + (P(),) * 8
    return jax.shard_map(body, mesh=mesh, in_specs=in_specs, out_specs=out_specs, check_vma=False)
```

```python
import functools

import jax
import jax.numpy as jnp
from jax import lax
from jax.experimental import pallas as pl
from jax.experimental.pallas import tpu as pltpu
from jax.sharding import PartitionSpec as P

BLOCK_LEN = 256
EPSILON = 1e-05
LANES = 128
HALO = 8
FAR = -1e30
F32 = jnp.float32
BF16 = jnp.bfloat16
CONTRACT_LAST = (((1,), (1,)), ((), ()))
CONTRACT_FIRST = (((0,), (0,)), ((), ()))


def mm(a, b):
    return jnp.dot(a, b, preferred_element_type=F32)


def mm_nt(a, b):
    return lax.dot_general(a, b, CONTRACT_LAST, preferred_element_type=F32)


def mm_tn(a, b):
    return lax.dot_general(a, b, CONTRACT_FIRST, preferred_element_type=F32)


def split_two(v):
    high = v.astype(BF16)
    return high, (v - high.astype(F32)).astype(BF16)


def split_three(v):
    first = v.astype(BF16)
    rest = v - first.astype(F32)
    second = rest.astype(BF16)
    return first, second, (rest - second.astype(F32)).astype(BF16)


def lanes_of(shape):
    return lax.broadcasted_iota(jnp.int32, shape, 1)


def rows_of(shape):
    return lax.broadcasted_iota(jnp.int32, shape, 0)


def spread_heads(v, spread, heads):
    first, second, third = split_three(v)
    lane = lanes_of(v.shape)
    packed = jnp.where(lane < heads, first.astype(F32), second.astype(F32))
    packed = jnp.where(lane < 2 * heads, packed, third.astype(F32))
    return mm(packed.astype(BF16), spread)


def head_sums(v, gather):
    high, low = split_two(v)
    return mm(high, gather) + mm(low, gather)


def tri_sums(tri, v):
    first, second, third = split_three(v)
    return mm(tri, first) + mm(tri, second) + mm(tri, third)


def spread_matrix(heads, channels):
    lane = rows_of((LANES, channels))
    head = lanes_of((LANES, channels)) // (channels // heads)
    return jnp.where((lane < 3 * heads) & (lane % heads == head), 1.0, 0.0).astype(BF16)


def gather_matrix(heads, channels):
    head = rows_of((channels, LANES)) // (channels // heads)
    return jnp.where(lanes_of((channels, LANES)) % heads == head, 1.0, 0.0).astype(BF16)


def conv_pre(buf, taps, length, tap_count):
    pre = taps[tap_count : tap_count + 1]
    for k in range(tap_count):
        pre = pre + taps[k : k + 1] * buf[pl.ds(HALO - tap_count + 1 + k, length), :]
    return pre


def fill(buf, prev_ref, cur_ref, is_first):
    prev = prev_ref[...]
    buf[0:HALO, :] = jnp.where(is_first, jnp.zeros_like(prev), prev)
    buf[HALO:, :] = cur_ref[...]


def step_values(dt_ref, ph):
    shifted = dt_ref[...] + ph[0:1]
    step_dt = jnp.maximum(shifted, 0.0) + jnp.log1p(jnp.exp(-jnp.abs(shifted)))
    log_step = step_dt * ph[1:2]
    return shifted, step_dt, log_step


def fwd_kernel(heads, gate_ref, xprev_ref, x_ref, bcprev_ref, bc_ref, dt_ref, gm_ref, px_ref, pbc_ref, ph_ref,
               mixed_ref, states_ref, sums_ref, xbuf, bcbuf, state, y_ref):
    step = pl.program_id(0)
    is_first = step == 0
    length, channels = x_ref.shape
    half = length // 2
    state_count = bc_ref.shape[1] // 2
    width = channels // heads

    @pl.when(is_first)
    def _():
        state[...] = jnp.zeros_like(state)

    fill(xbuf, xprev_ref, x_ref, is_first)
    fill(bcbuf, bcprev_ref, bc_ref, is_first)
    px, pbc, ph = px_ref[...], pbc_ref[...], ph_ref[...]
    x_low = jax.nn.silu(conv_pre(xbuf, px, length, 4)).astype(BF16)
    bc_low = jax.nn.silu(conv_pre(bcbuf, pbc, length, 4)).astype(BF16)
    b_low, c_low = bc_low[:, :state_count], bc_low[:, state_count:]
    _, step_dt, log_step = step_values(dt_ref, ph)
    tri = (rows_of((length, length)) >= lanes_of((length, length))).astype(F32).astype(BF16)
    cum = tri_sums(tri, log_step)
    cum_t = cum.T
    dt_t = step_dt.T
    spread = spread_matrix(heads, channels)
    exp_cum = spread_heads(jnp.exp(cum), spread, heads)
    weight = spread_heads(jnp.exp(cum[length - 1 : length] - cum) * step_dt, spread, heads)

    scores = mm_nt(c_low, b_low)
    lane = lanes_of((length, LANES))
    per_lane = LANES // width
    for group in range(heads // per_lane):
        cols = slice(group * LANES, (group + 1) * LANES)
        xp = x_low[:, cols]
        top = jnp.zeros((half, LANES), F32)
        bottom = jnp.zeros((half, LANES), F32)
        for s in range(per_lane):
            h = group * per_lane + s
            xm = jnp.where(lane // width == s, xp, jnp.zeros_like(xp))
            for part in range(2):
                r0, cn = part * half, (part + 1) * half
                rows = slice(r0, r0 + half)
                gaps = cum[rows, h : h + 1] - cum_t[h : h + 1, :cn]
                shape = (half, cn)
                keep = rows_of(shape) + r0 >= lanes_of(shape)
                decay = jnp.exp(jnp.where(keep, gaps, FAR))
                w = (scores[rows, :cn] * decay * dt_t[h : h + 1, :cn]).astype(BF16)
                if part == 0:
                    top = top + mm(w, xm[:cn])
                else:
                    bottom = bottom + mm(w, xm[:cn])
        y_ref[0:half, cols] = top
        y_ref[half:, cols] = bottom

    old = state[...]
    states_ref[0] = old
    old_high, old_low = split_two(old)
    carried = mm(c_low, old_high) + mm(c_low, old_low)
    x_wide = x_low.astype(F32)
    xw_high, xw_low = split_two(x_wide * weight)
    state[...] = old * exp_cum[length - 1 : length] + (mm_tn(b_low, xw_high) + mm_tn(b_low, xw_low))
    mixed = y_ref[...] + carried * exp_cum + px[6:7] * x_wide
    mixed_ref[...] = mixed
    gated = mixed * jax.nn.silu(gate_ref[...])
    squares = jnp.sum(gated * gated, axis=1, keepdims=True)
    inner = jnp.sum(gm_ref[...].astype(F32) * px[5:6] * gated, axis=1, keepdims=True)
    both = jnp.where(lane == 0, squares, jnp.where(lane == 1, inner, 0.0))
    sums_ref[0] = both.T[:8]


def bwd_kernel(heads, gate_ref, xprev_ref, x_ref, bcprev_ref, bc_ref, dt_ref, gm_ref, mixed_ref, states_ref, stats_ref,
               px_ref, pbc_ref, ph_ref, g_ref, gx_ref, gbc_ref, gh_ref, xbuf, bcbuf, gxbuf, gbcbuf, dstate, dx_ref, dg_ref):
    step = pl.program_id(0)
    is_first = step == pl.num_programs(0) - 1
    length, channels = x_ref.shape
    half = length // 2
    state_count = bc_ref.shape[1] // 2
    width = channels // heads

    @pl.when(step == 0)
    def _():
        dstate[...] = jnp.zeros_like(dstate)
        gxbuf[...] = jnp.zeros_like(gxbuf)
        gbcbuf[...] = jnp.zeros_like(gbcbuf)
        gx_ref[...] = jnp.zeros_like(gx_ref)
        gbc_ref[...] = jnp.zeros_like(gbc_ref)
        gh_ref[...] = jnp.zeros_like(gh_ref)

    fill(xbuf, xprev_ref, x_ref, is_first)
    fill(bcbuf, bcprev_ref, bc_ref, is_first)
    px, pbc, ph = px_ref[...], pbc_ref[...], ph_ref[...]
    pre_x = conv_pre(xbuf, px, length, 4)
    sig_x = jax.nn.sigmoid(pre_x)
    x_low = (pre_x * sig_x).astype(BF16)
    slope_x = sig_x * (1.0 + pre_x * (1.0 - sig_x))
    pre_bc = conv_pre(bcbuf, pbc, length, 4)
    sig_bc = jax.nn.sigmoid(pre_bc)
    bc_low = (pre_bc * sig_bc).astype(BF16)
    slope_bc = sig_bc * (1.0 + pre_bc * (1.0 - sig_bc))
    b_low, c_low = bc_low[:, :state_count], bc_low[:, state_count:]
    shifted, step_dt, log_step = step_values(dt_ref, ph)
    tri = (rows_of((length, length)) >= lanes_of((length, length))).astype(F32).astype(BF16)
    cum = tri_sums(tri, log_step)
    cum_t = cum.T
    spread = spread_matrix(heads, channels)
    gather = gather_matrix(heads, channels)
    exp_cum = spread_heads(jnp.exp(cum), spread, heads)
    weight = spread_heads(jnp.exp(cum[length - 1 : length] - cum) * step_dt, spread, heads)
    dt_wide = spread_heads(step_dt, spread, heads)
    x_wide = x_low.astype(F32)

    stats = stats_ref[0]
    stats = jnp.concatenate([stats, jnp.zeros((LANES - 8, length), F32)], axis=0).T
    rs, coef = stats[:, 0:1], stats[:, 1:2]
    gate = gate_ref[...]
    sig = jax.nn.sigmoid(gate)
    silu = gate * sig
    mixed = mixed_ref[...]
    gated = mixed * silu
    gm = gm_ref[...].astype(F32)
    ggated = rs * (gm * px[5:6]) - gated * coef
    d_gain = jnp.sum(gm * gated * rs, axis=0, keepdims=True)
    dy = ggated * silu
    g_ref[:, 0:channels] = (ggated * mixed * (sig * (1.0 + gate * (1.0 - sig)))).astype(BF16)
    dy_low = dy.astype(BF16)
    d_skip = jnp.sum(dy * x_wide, axis=0, keepdims=True)

    old = states_ref[0]
    old_high, old_low = split_two(old)
    ds = dstate[...]
    ds_high, ds_low = split_two(ds)
    dye = dy * exp_cum
    dye_low = dye.astype(BF16)
    dc = mm_nt(dye_low, old_high)
    carried = mm(c_low, old_high) + mm(c_low, old_low)
    from_carried = head_sums(dye * carried, gather)
    dxs = (mm(b_low, ds_high) + mm(b_low, ds_low)) * weight
    from_state = head_sums(x_wide * dxs, gather)
    db = mm_nt((x_wide * weight).astype(BF16), ds_high)
    last = exp_cum[length - 1 : length]
    decayed = jnp.sum(old * ds, axis=0, keepdims=True) * last
    decayed = head_sums(jnp.broadcast_to(decayed, (8, channels)), gather)[0:1]
    dstate[...] = ds * last + mm_tn(c_low, dye_low)

    scores = mm_nt(b_low, c_low)
    xdt_low = (x_wide * dt_wide).astype(BF16)
    lane = lanes_of((length, LANES))
    per_lane = LANES // width
    dg_ref[...] = jnp.zeros_like(dg_ref)
    col_sums = jnp.zeros((length, LANES), F32)
    row_sums = jnp.zeros((8, length), F32)
    row8 = rows_of((8, length))
    for group in range(heads // per_lane):
        cols = slice(group * LANES, (group + 1) * LANES)
        xp, dyp = xdt_low[:, cols], dy_low[:, cols]
        top = jnp.zeros((half, LANES), F32)
        bottom = jnp.zeros((half, LANES), F32)
        for s in range(per_lane):
            h = group * per_lane + s
            mine = lane // width == s
            xm = jnp.where(mine, xp, jnp.zeros_like(xp))
            dym = jnp.where(mine, dyp, jnp.zeros_like(dyp))
            col_parts = []
            row_parts = []
            for part in range(2):
                r0 = part * half
                rows = slice(r0, r0 + half)
                gaps = cum_t[h : h + 1, r0:] - cum[rows, h : h + 1]
                shape = (half, length - r0)
                keep = lanes_of(shape) >= rows_of(shape)
                decay = jnp.exp(jnp.where(keep, gaps, FAR))
                v = scores[rows, r0:] * decay
                dw = mm_nt(xm[rows], dyp[r0:])
                dg_ref[rows, r0:] += decay * dw
                e = v * dw
                col_parts.append(jnp.sum(e, axis=1, keepdims=True))
                row_parts.append(jnp.sum(e, axis=0, keepdims=True))
                if part == 0:
                    top = top + mm(v.astype(BF16), dym)
                else:
                    bottom = bottom + mm(v.astype(BF16), dym[r0:])
            col = jnp.concatenate(col_parts, axis=0)
            row = row_parts[0] + jnp.concatenate([jnp.zeros((1, half), F32), row_parts[1]], axis=1)
            col_sums = jnp.where(lane % heads == h, col, col_sums)
            row_sums = jnp.where(row8 == h, row, row_sums)
        dx_ref[0:half, cols] = top
        dx_ref[half:, cols] = bottom

    dg_low = dg_ref[...].astype(BF16)
    db = db + mm(dg_low, c_low)
    dc = dc + mm_tn(dg_low, b_low)
    dx = dx_ref[...] * dt_wide + dxs + px[6:7] * dy

    row_cols = jnp.concatenate([row_sums] * (LANES // 8), axis=0).T
    local = row_cols - col_sums + from_carried - from_state
    tri_up = (rows_of((length, length)) <= lanes_of((length, length))).astype(F32).astype(BF16)
    grad_log = tri_sums(tri_up, local) + (jnp.sum(from_state, axis=0, keepdims=True) + decayed)
    direct = jnp.where(step_dt > 0.0, (col_sums + from_state) / step_dt, 0.0)
    grad_dt = (direct + ph[1:2] * grad_log) * jax.nn.sigmoid(shifted)
    gh_ref[0:1] += jnp.sum(grad_dt, axis=0, keepdims=True)
    gh_ref[1:2] += jnp.sum(grad_log * log_step, axis=0, keepdims=True)
    g_ref[:, 2 * channels + 2 * state_count :] = jnp.where(lane < heads, grad_dt, 0.0).astype(BF16)

    def conv_back(grad, slope, buf, gbuf, taps, sums_ref):
        gbuf[length:, :] = gbuf[0:HALO, :]
        gp = grad * slope
        gbuf[0:length, :] = gp
        result = jnp.zeros_like(gp)
        for k in range(4):
            result = result + taps[k : k + 1] * gbuf[pl.ds(3 - k, length), :]
            sums_ref[k : k + 1] += jnp.sum(buf[pl.ds(HALO - 3 + k, length), :] * gp, axis=0, keepdims=True)
        sums_ref[4:5] += jnp.sum(gp, axis=0, keepdims=True)
        return result.astype(BF16)

    g_ref[:, channels : 2 * channels] = conv_back(dx, slope_x, xbuf, gxbuf, px, gx_ref)
    g_ref[:, 2 * channels : 2 * channels + 2 * state_count] = conv_back(
        jnp.concatenate([db, dc], axis=1), slope_bc, bcbuf, gbcbuf, pbc, gbc_ref
    )
    gx_ref[5:6] += d_gain
    gx_ref[6:7] += d_skip


def scan_specs(length, channels, states, block):
    halo = length // HALO

    def at(width, start):
        return pl.BlockSpec((length, width), lambda i: (block(i), start // width))

    def before(width, start):
        return pl.BlockSpec((HALO, width), lambda i: (jnp.maximum(block(i) * halo - 1, 0), start // width))

    return [
        at(channels, 0),
        before(channels, channels),
        at(channels, channels),
        before(2 * states, 2 * channels),
        at(2 * states, 2 * channels),
        at(LANES, 2 * channels + 2 * states),
    ]


def whole(shape):
    return pl.BlockSpec(shape, lambda i: (0,) * len(shape))


def mix_forward(proj, grad_mixed, px, pbc, ph, heads):
    tokens, channels = grad_mixed.shape
    states = pbc.shape[1] // 2
    length = BLOCK_LEN
    blocks = tokens // length
    block = lambda i: i
    return pl.pallas_call(
        functools.partial(fwd_kernel, heads),
        grid=(blocks,),
        in_specs=scan_specs(length, channels, states, block)
        + [pl.BlockSpec((length, channels), lambda i: (i, 0)), whole(px.shape), whole(pbc.shape), whole(ph.shape)],
        out_specs=[
            pl.BlockSpec((length, channels), lambda i: (i, 0)),
            pl.BlockSpec((1, states, channels), lambda i: (i, 0, 0)),
            pl.BlockSpec((1, 8, length), lambda i: (i, 0, 0)),
        ],
        out_shape=[
            jax.ShapeDtypeStruct((tokens, channels), F32),
            jax.ShapeDtypeStruct((blocks, states, channels), F32),
            jax.ShapeDtypeStruct((blocks, 8, length), F32),
        ],
        scratch_shapes=[
            pltpu.VMEM((length + HALO, channels), F32),
            pltpu.VMEM((length + HALO, 2 * states), F32),
            pltpu.VMEM((states, channels), F32),
            pltpu.VMEM((length, channels), F32),
        ],
        name="mix_forward",
    )(proj, proj, proj, proj, proj, proj, grad_mixed, px, pbc, ph)


def mix_backward(proj, grad_mixed, mixed, states_in, stats, px, pbc, ph, heads):
    tokens, channels = grad_mixed.shape
    states = pbc.shape[1] // 2
    length = BLOCK_LEN
    blocks = tokens // length
    block = lambda i: blocks - 1 - i
    total = 2 * channels + 2 * states + LANES
    return pl.pallas_call(
        functools.partial(bwd_kernel, heads),
        grid=(blocks,),
        in_specs=scan_specs(length, channels, states, block)
        + [
            pl.BlockSpec((length, channels), lambda i: (block(i), 0)),
            pl.BlockSpec((length, channels), lambda i: (block(i), 0)),
            pl.BlockSpec((1, states, channels), lambda i: (block(i), 0, 0)),
            pl.BlockSpec((1, 8, length), lambda i: (block(i), 0, 0)),
            whole(px.shape),
            whole(pbc.shape),
            whole(ph.shape),
        ],
        out_specs=[
            pl.BlockSpec((length, total), lambda i: (block(i), 0)),
            whole((8, channels)),
            whole((8, 2 * states)),
            whole((8, LANES)),
        ],
        out_shape=[
            jax.ShapeDtypeStruct((tokens, total), BF16),
            jax.ShapeDtypeStruct((8, channels), F32),
            jax.ShapeDtypeStruct((8, 2 * states), F32),
            jax.ShapeDtypeStruct((8, LANES), F32),
        ],
        scratch_shapes=[
            pltpu.VMEM((length + HALO, channels), F32),
            pltpu.VMEM((length + HALO, 2 * states), F32),
            pltpu.VMEM((length + HALO, channels), F32),
            pltpu.VMEM((length + HALO, 2 * states), F32),
            pltpu.VMEM((states, channels), F32),
            pltpu.VMEM((length, channels), F32),
            pltpu.VMEM((length, length), F32),
        ],
        name="mix_backward",
    )(proj, proj, proj, proj, proj, proj, grad_mixed, mixed, states_in, stats, px, pbc, ph)


MESH = pl.DeviceIdType.MESH
PIECES = 4


def remote(src, dst, send_sem, recv_sem, target):
    return pltpu.make_async_remote_copy(
        src_ref=src, dst_ref=dst, send_sem=send_sem, recv_sem=recv_sem, device_id=target, device_id_type=MESH
    )


def head_kernel(lines, hid_in, grad_in, win_in, wo_in, proj_out, gm_out, hid_out, hid_t_out, grad_out, win_out, wo_out,
                hbuf, htbuf, gbuf, winbuf, wobuf, pbuf, mbuf, a_send, a_recv, w_send, w_recv, y_send, y_recv, l_sem, p_sem):
    rank = lax.axis_index("tensor")
    place = lax.axis_index("dp")
    z, y = place // 2, place % 2
    core, chip = rank % 2, rank // 2
    partner = {"tensor": chip * 2 + (1 - core)}
    across = {"tensor": (1 - chip) * 2 + core}
    beside = {"dp": z * 2 + (1 - y)}
    above = {"dp": place + 2}
    below = {"dp": place - 2}
    tokens = hid_in.shape[0]
    piece = tokens // PIECES

    barrier = pltpu.get_barrier_semaphore()
    for target in (partner, across, beside):
        pl.semaphore_signal(barrier, inc=1, device_id=target, device_id_type=MESH)

    @pl.when(z < lines - 1)
    def _():
        pl.semaphore_signal(barrier, inc=1, device_id=above, device_id_type=MESH)

    @pl.when(z > 0)
    def _():
        pl.semaphore_signal(barrier, inc=1, device_id=below, device_id_type=MESH)

    weights = ((win_in, winbuf), (wo_in, wobuf))

    def block_rows(owner, c):
        return pl.ds(pl.multiple_of(owner * tokens + c * piece, piece), piece)

    locals_ = []

    def local(src, dst, k):
        copy = pltpu.make_async_copy(src, dst, l_sem.at[k])
        copy.start()
        return copy

    own_rows = pl.ds(pl.multiple_of(rank * tokens, tokens), tokens)
    own_h = local(hid_in, hbuf.at[own_rows], 0)
    own_g = local(grad_in, gbuf.at[own_rows], 1)
    own_w = []
    for w, (src, dst) in enumerate(weights):
        rows = src.shape[0]
        own_w.append(local(src, dst.at[pl.ds(pl.multiple_of(place * rows, rows), rows)], 2 + w))

    neighbours = 3 + (z + lines - 1) // lines + (2 * lines - 2 - z) // lines
    pl.semaphore_wait(barrier, neighbours)

    def token_copy(a, kind, c):
        src_in, buf = ((hid_in, hbuf), (grad_in, gbuf))[a]
        if kind == 2:
            owner = (1 - chip) * 2 + core
            src = buf.at[block_rows(owner, c)]
        else:
            owner = rank
            src = src_in.at[pl.ds(c * piece, piece)]
        return remote(src, buf.at[block_rows(owner, c)], a_send.at[a, kind, c], a_recv.at[a, kind, c],
                      across if kind == 1 else partner)

    def shard(w, source, half):
        src, dst = weights[w]
        rows = src.shape[0] // 2
        return dst.at[pl.ds(pl.multiple_of((source * 2 + y) * 2 * rows + half * rows, rows), rows)]

    def shard_source(w, side, far, half):
        if far == 0:
            src, _ = weights[w]
            rows = src.shape[0] // 2
            return z, src.at[pl.ds(half * rows, rows)]
        source = z - far if side == 0 else z + far
        return source, shard(w, source, half)

    def line_copy(w, side, far, half):
        source, src = shard_source(w, side, far, half)
        return remote(src, shard(w, source, half), w_send.at[w, side, far, half], w_recv.at[w, side, far + 1, half],
                      above if side == 0 else below)

    def beside_copy(w, side, far, half):
        source, src = shard_source(w, side, far, half)
        return remote(src, shard(w, source, half), y_send.at[w, side, far, half], y_recv.at[w, side, far, half], beside)

    def has(side, far):
        return z - far >= 0 if side == 0 else z + far <= lines - 1

    def goes_on(side, far):
        if side == 0:
            return (z - far >= 0) & (z < lines - 1)
        return (z + far <= lines - 1) & (z > 0)

    def send_shard(w, far, half):
        for side in range(2):
            if far == 0:
                pl.when(goes_on(side, 0))(lambda side=side: line_copy(w, side, 0, half).start())
            else:
                def arrive(side=side):
                    line_copy(w, side, far - 1, half).wait_recv()
                    pl.when(goes_on(side, far))(lambda: line_copy(w, side, far, half).start())
                    beside_copy(w, side, far, half).start()
                pl.when(has(side, far))(arrive)
        if far == 0:
            beside_copy(w, 0, 0, half).start()

    for half in range(2):
        send_shard(0, 0, half)
    for c in range(PIECES):
        token_copy(0, 1, c).start()
    for c in range(PIECES):
        token_copy(0, 0, c).start()

    def pass_on(a, c):
        token_copy(a, 1, c).wait_recv()
        token_copy(a, 2, c).start()

    events = []
    for far in range(1, lines):
        for half in range(2):
            events.append(functools.partial(send_shard, 0, far, half))
    for c in range(PIECES):
        def step(c=c):
            pass_on(0, c)
            token_copy(1, 1, c).start()
        events.insert(min(2 * c + 1, len(events)), step)
    for event in events:
        event()
    for far in range(lines):
        for half in range(2):
            send_shard(1, far, half)
    for c in range(PIECES):
        token_copy(1, 0, c).start()

    own_h.wait()
    for c in range(PIECES):
        token_copy(0, 0, c).wait_recv()
        token_copy(0, 2, c).wait_recv()

    def each_beside(w, act):
        for far in range(lines):
            for side in range(2):
                if far == 0 and side == 1:
                    continue
                def go(side=side, far=far):
                    for half in range(2):
                        act(beside_copy(w, side, far, half))
                pl.when(has(side, far))(go)

    own_w[0].wait()
    each_beside(0, lambda copy: copy.wait_recv())
    outs = [local(hbuf, hid_out, 0), local(winbuf, win_out, 2)]

    total = hbuf.shape[0]
    block = pbuf.shape[1]
    done = []
    for b in range(total // block):
        slot = b % 2
        rows = pl.ds(b * block, block)
        if b >= 2:
            done[b - 2].wait()
        pbuf[slot] = mm(hbuf[rows, :], winbuf[...])
        copy = pltpu.make_async_copy(pbuf.at[slot], proj_out.at[rows], p_sem.at[slot])
        copy.start()
        done.append(copy)
        htbuf[:, rows] = hbuf[rows, :].T
        if b % 2 == 1 and b // 2 < PIECES:
            pass_on(1, b // 2)
    outs.append(local(htbuf, hid_t_out, 4))
    own_g.wait()
    own_w[1].wait()
    each_beside(1, lambda copy: copy.wait_recv())
    outs.append(local(wobuf, wo_out, 3))
    for c in range(PIECES):
        token_copy(1, 0, c).wait_recv()
        token_copy(1, 2, c).wait_recv()
    outs.append(local(gbuf, grad_out, 1))
    for b in range(total // block):
        rows = pl.ds(b * block, block)
        mbuf[rows, :] = mm(gbuf[rows, :], wobuf[...]).astype(BF16)
    outs.append(local(mbuf, gm_out, 5))

    for copy in outs + done[-2:]:
        copy.wait()
    for a in range(2):
        for kind in range(3):
            for c in range(PIECES):
                token_copy(a, kind, c).wait_send()
    for w in range(2):
        each_beside(w, lambda copy: copy.wait_send())
        for far in range(lines - 1):
            for side in range(2):
                def go(side=side, far=far):
                    for half in range(2):
                        line_copy(w, side, far, half).wait_send()
                pl.when(goes_on(side, far))(go)


def gather_and_project(hidden, grads, w_in, w_o, lines):
    parts = lax.axis_size("tensor")
    tokens, features = hidden.shape
    rows, side = w_in.shape
    channels = w_o.shape[1]
    total = tokens * parts
    any_spec = pl.BlockSpec(memory_space=pl.ANY)
    shapes = [
        ((total, side), F32), ((total, channels), BF16), ((total, features), BF16), ((features, total), BF16),
        ((total, features), BF16), ((2 * lines * rows, side), BF16), ((2 * lines * rows, channels), BF16),
    ]
    return pl.pallas_call(
        functools.partial(head_kernel, lines),
        in_specs=[any_spec] * 4,
        out_specs=[any_spec] * len(shapes),
        out_shape=[jax.ShapeDtypeStruct(*s) for s in shapes],
        scratch_shapes=[
            pltpu.VMEM((total, features), BF16),
            pltpu.VMEM((features, total), BF16),
            pltpu.VMEM((total, features), BF16),
            pltpu.VMEM((2 * lines * rows, side), BF16),
            pltpu.VMEM((2 * lines * rows, channels), BF16),
            pltpu.VMEM((2, BLOCK_LEN, side), F32),
            pltpu.VMEM((total, channels), BF16),
            pltpu.SemaphoreType.DMA((2, 3, PIECES)),
            pltpu.SemaphoreType.DMA((2, 3, PIECES)),
            pltpu.SemaphoreType.DMA((2, 2, lines, 2)),
            pltpu.SemaphoreType.DMA((2, 2, lines + 1, 2)),
            pltpu.SemaphoreType.DMA((2, 2, lines, 2)),
            pltpu.SemaphoreType.DMA((2, 2, lines, 2)),
            pltpu.SemaphoreType.DMA((6,)),
            pltpu.SemaphoreType.DMA((2,)),
        ],
        compiler_params=pltpu.CompilerParams(collective_id=0, has_side_effects=True),
        name="gather_and_project",
    )(hidden, grads, w_in, w_o)


def widen(piece, start, full_size):
    holder = jnp.zeros(piece.shape[:-1] + (full_size,), F32)
    return lax.dynamic_update_slice_in_dim(holder, piece, start, piece.ndim - 1)


def body(acts, grad_out, norm_gain, w_zx, w_bc, w_dt, w_out, conv_x, conv_x_bias, conv_bc, conv_bc_bias,
         dt_bias, a_log, d_skip, gate_gain):
    parts = lax.axis_size("tensor")
    rank = lax.axis_index("tensor")
    rows, features = acts.shape[1:]
    w_rows, _, channels = w_zx.shape
    heads = w_dt.shape[1]
    states = w_bc.shape[1] // 2
    width = channels // heads
    total_channels, total_heads = channels * parts, heads * parts
    chan_start, head_start = rank * channels, rank * heads
    repeat = LANES // heads

    acts_row = acts[0].astype(F32)
    rs0 = lax.rsqrt(jnp.mean(acts_row * acts_row, axis=-1, keepdims=True) + EPSILON)
    local_w = jnp.concatenate([w_zx.reshape(w_rows, 2 * channels), w_bc, jnp.tile(w_dt, (1, repeat))], axis=1)
    proj, grad_mixed, hidden, hidden_t, grad_rows, w_in, w_o = gather_and_project(
        (acts_row * rs0 * norm_gain).astype(BF16), grad_out[0], local_w, w_out, lax.axis_size("dp") // 2
    )

    def take(v, start, size):
        return lax.dynamic_slice_in_dim(v, start, size, v.ndim - 1)

    gain = take(gate_gain, chan_start, channels)
    skip = jnp.repeat(take(d_skip, head_start, heads), width)
    px = jnp.concatenate(
        [take(conv_x, chan_start, channels), take(conv_x_bias, chan_start, channels)[None], gain[None], skip[None],
         jnp.zeros((1, channels), F32)], axis=0)
    pbc = jnp.concatenate([conv_bc, conv_bc_bias[None], jnp.zeros((3, 2 * states), F32)], axis=0)
    ph = jnp.stack([jnp.tile(take(dt_bias, head_start, heads), repeat),
                    jnp.tile(-jnp.exp(take(a_log, head_start, heads)), repeat)])
    ph = jnp.concatenate([ph, jnp.zeros((6, LANES), F32)], axis=0)

    mixed, state_in, sums = mix_forward(proj, grad_mixed, px, pbc, ph, heads)
    sums = lax.psum(sums[:, :2], "tensor")
    inv = lax.rsqrt(sums[:, 0] / total_channels + EPSILON)
    coef = inv * inv * inv * (sums[:, 1] / total_channels)
    stats = jnp.concatenate([jnp.stack([inv, coef], axis=1), jnp.zeros((inv.shape[0], 6, inv.shape[1]), F32)], axis=1)
    mixed_out = (mixed * jax.nn.silu(proj[:, :channels]) * inv.reshape(-1, 1) * gain).astype(BF16)
    projected = lax.psum_scatter(mm_nt(mixed_out, w_o).astype(BF16), "tensor", scatter_dimension=0, tiled=True)
    out_acts = (acts_row + projected.astype(F32)).astype(BF16)[None]
    grad_w_out = lax.psum_scatter(mm_tn(grad_rows, mixed_out).astype(BF16), "dp", scatter_dimension=0, tiled=True)

    g_all, gx, gbc, gh = mix_backward(proj, grad_mixed, mixed, state_in, stats, px, pbc, ph, heads)
    grad_hidden = lax.psum_scatter(mm_nt(g_all, w_in).astype(BF16), "tensor", scatter_dimension=0, tiled=True)
    grad_w = lax.psum_scatter(mm_tn(hidden, g_all).astype(BF16), "dp", scatter_dimension=0, tiled=True).astype(F32)
    grad_w_bc = lax.psum(grad_w[:, 2 * channels : 2 * channels + 2 * states], "tensor")

    grad_hidden = grad_hidden.astype(F32)
    grad_ng = jnp.sum(grad_hidden * acts_row * rs0, axis=0)
    pulled = grad_hidden * norm_gain
    inner = jnp.sum(pulled * acts_row, axis=-1, keepdims=True)
    grad_acts = grad_out[0].astype(F32) + pulled * rs0 - acts_row * (rs0 * rs0 * rs0 / features * inner)

    pieces = (
        grad_ng,
        widen(gx[0:4], chan_start, total_channels),
        widen(gx[4], chan_start, total_channels),
        gbc[0:4],
        gbc[4],
        widen(gh[0, :heads], head_start, total_heads),
        widen(gh[1, :heads], head_start, total_heads),
        widen(jnp.sum(gx[6].reshape(heads, width), axis=1), head_start, total_heads),
        widen(gx[5], chan_start, total_channels),
    )
    ng, cx, cxb, cbc, cbcb, dtb, alog, dsk, gg = lax.psum(pieces, ("dp", "tensor"))
    return (
        out_acts,
        grad_acts[None],
        ng,
        grad_w[:, : 2 * channels].reshape(w_rows, 2, channels),
        grad_w_bc,
        grad_w[:, 2 * channels + 2 * states : 2 * channels + 2 * states + heads],
        grad_w_out.astype(F32),
        cx,
        cxb,
        cbc,
        cbcb,
        dtb,
        alog,
        dsk,
        gg,
    )


def solution(mesh):
    in_specs = (
        P("dp", "tensor", None),
        P("dp", "tensor", None),
        P(),
        P("dp", None, "tensor"),
        P("dp", None),
        P("dp", "tensor"),
        P("dp", "tensor"),
    ) + (P(),) * 8
    out_specs = (
        P("dp", "tensor", None),
        P("dp", "tensor", None),
        P(),
        P("dp", None, "tensor"),
        P("dp", None),
        P("dp", "tensor"),
        P("dp", "tensor"),
    ) + (P(),) * 8
    return jax.shard_map(body, mesh=mesh, in_specs=in_specs, out_specs=out_specs, check_vma=False)
```
